32 devices in a mesh: dp: 16 (over z, y, core), mp: 2 (over x).
Axes of the slice: x: 2, y: 2, z: 4, core: 2. Of those that a mesh axis runs over, the one named last changes fastest.
Arguments:
- activations: bfloat16 [8192, 1792], P('dp', 'mp'), may hold values from -6 to 6
- projection: bfloat16 [1792, 9216], P('mp', 'dp'), may hold values from -0.125 to 0.125
Outputs:
- projected: bfloat16 [8192, 9216], P('dp', 'mp')
The draws below stay inside these ranges and needn't reach their ends.
All inputs are finite; a program needn't handle non-finite values.
Results may differ from the reference program's by a relative error of at most 0.001.
Values may be sent and summed in bfloat16 or wider, within the bound.
No kernel may reach another device: no remote copies, remote signals or barrier semaphores. Data moves between devices by JAX's collectives and lax.ppermute only.
A program may use at most 128 MiB of HBM per device.

```python
import jax
import jax.numpy as jnp
from jax import lax

D_MP = 896
F = 9216
TOK_DEV = 512
D = 1792
TOKENS = 8192
N_DP = 16
N_MP = 2


def levels(key, dims, pieces, smallest, high):
    factor_of, own = 1.0, jax.random.fold_in(key, 6)
    for position, blocks in pieces:
        draws = jnp.exp(jax.random.uniform(jax.random.fold_in(own, position), (blocks,), jnp.float32, smallest / len(pieces), high / len(pieces)))
        factor_of = factor_of * jnp.repeat(draws, dims[position] // blocks).reshape([-1 if axis == position else 1 for axis in range(len(dims))])
    return factor_of


def normal_values(stream_key, dims, scale, limit, split=(), held_as=jnp.bfloat16):
    values = scale * jax.random.normal(stream_key, dims, jnp.float32)
    if split:
        values = values * levels(stream_key, dims, split, -0.22, 0.18)
    return jnp.clip(values, -limit, limit).astype(held_as)


def setup_inputs(seed: int = 0) -> dict:
    streams_of = jax.random.split(jax.random.key(seed), 3)
    return {
        "activations": normal_values(streams_of[0], (TOKENS, D), 1.0, 6.0, ((0, 16), (1, 2))),
        "projection": normal_values(streams_of[1], (D, F), D ** -0.5, 0.125, ((0, 2), (1, 16))),
    }


def reference(activations, projection):
    block_rows = TOK_DEV
    blocks = activations.reshape(N_DP, block_rows, D_MP * N_MP)

    def one_block(rows):
        return jnp.dot(rows, projection, preferred_element_type=jnp.float32).astype(jnp.bfloat16)

    result = lax.map(one_block, blocks)
    return result.reshape(N_DP * block_rows, F)
```

```python
import functools

import jax
import jax.numpy as jnp
from jax import lax
from jax.experimental import pallas as pl
from jax.experimental.pallas import tpu as pltpu
from jax.sharding import PartitionSpec as P


CHUNKS = 2
NAMES = ("O", "S", "B", "C")


def plain(activations, projection):
    wide_rows = lax.all_gather(activations, "mp", axis=1, tiled=True)
    local_cols = lax.all_to_all(projection, "mp", split_axis=1, concat_axis=0, tiled=True)
    finished = jnp.dot(
        wide_rows,
        lax.all_gather(local_cols, "dp", axis=1, tiled=True),
        preferred_element_type=jnp.float32,
    )
    finished = finished.astype(jnp.bfloat16)
    tok_rows = finished.shape[0]
    blocks = lax.axis_size("dp")
    share = local_cols.shape[1]
    sectioned = finished.reshape(tok_rows, blocks, 1, share)
    placed = lax.all_to_all(sectioned, "mp", split_axis=1, concat_axis=2, tiled=True)
    return placed.reshape(tok_rows, placed.shape[1] * placed.shape[2] * share)


def pairs(move):
    out = []
    for z in range(4):
        for y in range(2):
            for c in range(2):
                for x in range(2):
                    to = move(z, y, c, x)
                    if to is not None:
                        tz, ty, tc, tx = to
                        out.append((((z * 2 + y) * 2 + c) * 2 + x, ((tz * 2 + ty) * 2 + tc) * 2 + tx))
    return out


def send(array, move):
    return lax.ppermute(array, ("dp", "mp"), pairs(move))


def over_x(z, y, c, x):
    return z, y, c, 1 - x


def turn(z, y, c, x):
    return z, y, x, c


def pair_z(z, y, c, x):
    return z ^ 1, y, c, x


def middle(z, y, c, x):
    return (3 - z, y, c, x) if z in (1, 2) else None


def outward(z, y, c, x):
    return {1: (0, y, c, x), 2: (3, y, c, x)}.get(z)


def over_y(z, y, c, x):
    return z, 1 - y, c, x


def over_core(z, y, c, x):
    return z, y, 1 - c, x


def to_home(z, y, c, x):
    return (z, y, c, 1 - x) if x != z // 2 else None


def from_home(z, y, c, x):
    return (z, y, c, 1 - x) if x == z // 2 else None


def product_kernel(count, *refs):
    mine, other = refs[0], refs[1]
    weights = refs[2 : 2 + 2 * count]
    out = refs[2 + 2 * count]
    rows_a, rows_b, w_a, w_b, sems = refs[3 + 2 * count :]
    part = w_a.shape[0] // count
    copies = [
        pltpu.make_async_copy(mine, rows_a, sems.at[0]),
        pltpu.make_async_copy(other, rows_b, sems.at[1]),
    ]
    for h in range(count):
        copies.append(pltpu.make_async_copy(weights[h], w_a.at[pl.ds(h * part, part)], sems.at[2 + h]))
        copies.append(
            pltpu.make_async_copy(weights[count + h], w_b.at[pl.ds(h * part, part)], sems.at[2 + count + h])
        )
    for copy in copies:
        copy.start()
    for copy in copies:
        copy.wait()
    step = rows_a.shape[0] // 2
    dims = (((1,), (1,)), ((), ()))

    @pl.loop(0, 2)
    def _(i):
        at = pl.ds(pl.multiple_of(i * step, step), step)
        total = lax.dot_general(rows_a[at, :], w_a[...], dims, preferred_element_type=jnp.float32)
        total += lax.dot_general(rows_b[at, :], w_b[...], dims, preferred_element_type=jnp.float32)
        out[at, :] = total.astype(out.dtype)


def product(mine, other, near, far):
    count = len(near)
    rows, depth = mine.shape
    cols = sum(w.shape[0] for w in near)
    any_spec = pl.BlockSpec(memory_space=pl.ANY)
    return pl.pallas_call(
        functools.partial(product_kernel, count),
        out_shape=jax.ShapeDtypeStruct((rows, cols), mine.dtype),
        in_specs=[any_spec] * (2 + 2 * count),
        out_specs=pl.BlockSpec(memory_space=pltpu.VMEM),
        scratch_shapes=[
            pltpu.VMEM((rows, depth), mine.dtype),
            pltpu.VMEM((rows, depth), mine.dtype),
            pltpu.VMEM((cols, depth), mine.dtype),
            pltpu.VMEM((cols, depth), mine.dtype),
            pltpu.SemaphoreType.DMA((2 + 2 * count,)),
        ],
        compiler_params=pltpu.CompilerParams(vmem_limit_bytes=16 << 20),
        cost_estimate=pl.CostEstimate(
            flops=4 * rows * cols * depth,
            bytes_accessed=2 * (2 * rows * depth + 2 * cols * depth + rows * cols),
            transcendentals=0,
        ),
    )(mine, other, *near, *far)


def place_kernel(where, *refs):
    own, got = refs[0:8], refs[8:16]
    out, buf, sems = refs[16], refs[17], refs[18]
    home, x, parity, y = where[0], where[1], where[2], where[3]
    cols = buf.shape[3]
    for g in range(4):
        p, q = g // 2, g % 2
        pick = (1 - home) * 4 + 2 * jnp.abs(p - parity) + jnp.abs(q - y)
        for k in range(8):

            @pl.when(pick == k)
            def _(k=k, g=g):
                pltpu.make_async_copy(own[k], buf.at[g, x], sems.at[g, 0]).start()
                pltpu.make_async_copy(got[k], buf.at[g, 1 - x], sems.at[g, 1]).start()

    for g in range(4):
        pltpu.make_async_copy(own[0], buf.at[g, x], sems.at[g, 0]).wait()
        pltpu.make_async_copy(got[0], buf.at[g, 1 - x], sems.at[g, 1]).wait()
        out[:, 2 * cols * g : 2 * cols * (g + 1)] = jnp.concatenate([buf[g, 0], buf[g, 1]], axis=1)


def place(where, own, got):
    rows, cols = own[0].shape
    any_spec = pl.BlockSpec(memory_space=pl.ANY)
    return pl.pallas_call(
        place_kernel,
        out_shape=jax.ShapeDtypeStruct((rows, 8 * cols), own[0].dtype),
        in_specs=[pl.BlockSpec(memory_space=pltpu.SMEM)] + [any_spec] * 16,
        out_specs=pl.BlockSpec(memory_space=pltpu.VMEM),
        scratch_shapes=[
            pltpu.VMEM((4, 2, rows, cols), own[0].dtype),
            pltpu.SemaphoreType.DMA((4, 2)),
        ],
        compiler_params=pltpu.CompilerParams(vmem_limit_bytes=32 << 20),
        cost_estimate=pl.CostEstimate(flops=rows * cols * 8, bytes_accessed=32 * rows * cols, transcendentals=0),
    )(where, *own, *got)


def lined(activations, projection):
    x = lax.axis_index("mp")
    i = lax.axis_index("dp")
    c, y, z = i % 2, (i // 2) % 2, i // 4
    part = projection.shape[1] // CHUNKS

    weights = projection.T
    chunks = [send(weights[h * part : (h + 1) * part], turn) for h in range(CHUNKS)]
    other_rows = send(activations, over_x)
    same = x == c
    mine = jnp.where(same, activations, other_rows)
    other = jnp.where(same, other_rows, activations)
    inner = (z == 1) | (z == 2)

    held = {name: [None] * CHUNKS for name in NAMES}
    for h, own in enumerate(chunks):
        near = send(own, pair_z)
        mid_own = send(own, middle)
        mid_near = send(near, middle)
        held["O"][h] = own
        held["S"][h] = near
        held["B"][h] = jnp.where(inner, mid_own, send(mid_own, outward))
        held["C"][h] = jnp.where(inner, mid_near, send(mid_near, outward))
    blocks = []
    for name in NAMES:
        blocks.append(held[name])
        blocks.append([send(w, over_y) for w in held[name]])

    own, got = [], []
    for k, block in enumerate(blocks):
        piece = product(mine, other, block, [send(w, over_core) for w in block])
        own.append(piece)
        got.append(send(piece, to_home if k < 4 else from_home))
    home = (x == z // 2).astype(jnp.int32)
    parity = jnp.where(home == 1, z % 2, z // 2)
    where = jnp.stack([home, x, parity, y]).astype(jnp.int32)
    return place(where, own, got)


def solution(mesh):
    fits = mesh.shape["dp"] == 16 and mesh.shape["mp"] == 2
    placed = (P("dp", "mp"), P("mp", "dp"))
    return jax.shard_map(
        lined if fits else plain, mesh=mesh, in_specs=placed, out_specs=P("dp", "mp"), check_vma=False
    )
```
